256 devices in a mesh: row: 8 (over y, core), col: 32 (over x, z).
Axes of the slice: x: 4, y: 4, z: 8, core: 2. Of those that a mesh axis runs over, the one named last changes fastest.
Arguments:
- x_blocks: bfloat16 [8, 32, 42, 128, 128], P('row', 'col'), may hold values from -1.1953125 to 1.1953125
- x_slots: int32 [8, 32, 42], replicated, may hold values from 0 to 255, as said below
- x_count: int32 [8, 32], replicated, may hold values from 21 to 42, as said below
- s_slots: int32 [8, 32, 2], replicated, may hold values from 0 to 15, as said below
- s_count: int32 [8, 32], replicated, may hold values from 1 to 2, as said below
Outputs:
- square_blocks: bfloat16 [8, 32, 2, 128, 128], P('row', 'col')
- result_blocks: bfloat16 [8, 32, 2, 128, 128], P('row', 'col')
The draws below stay inside these ranges and needn't reach their ends.
Inputs may be any that keep to these rules, and one draw needn't show every extreme that they name: `x_slots`: in each tile the live slots hold distinct positions; the live blocks whose position % 32 is below 2 come first among the live slots, at most 2 of them, and some tile has exactly 2. Positions of slots that are not live are arbitrary within the range. `x_count`: some tile has exactly 42 live slots. `s_slots`: in each tile the live slots hold distinct positions. `s_count`: some tile has exactly 2 live slots.
All inputs are finite; a program needn't handle non-finite values.
Results may differ from the reference program's by a relative error of at most 0.0049.
Values may be sent and summed in bfloat16 or wider, within the bound.
A program may use at most 128 MiB of HBM per device.

```python
import jax
import jax.numpy as jnp
from jax import lax

BLOCK = 128
RB = 8
JW = 2
NB = 256
KB = 32
CAPW = 2
CAPX = 42
CAPS = 2
N_ROW = 8
N_COL = 32


def tile_layout(key):
    tile_total = N_ROW * N_COL
    base_key = jax.random.fold_in(key, 41)
    keys_all = jax.random.split(base_key, 7)
    lowest = CAPX // 2
    x_total = jax.random.randint(keys_all[0], (tile_total,), lowest, CAPX + 1)
    window_total = jax.random.randint(keys_all[1], (tile_total,), 0, CAPW + 1)
    chosen = jax.random.randint(keys_all[2], (2,), 0, tile_total)
    x_total = x_total.at[chosen[0]].set(CAPX)
    window_total = window_total.at[chosen[1]].set(CAPW)
    window_total = jnp.minimum(window_total, x_total)
    window_cells = RB * JW
    other_cells = RB * (KB - JW)
    near_range = jnp.arange(window_cells, dtype=jnp.int32)
    far_range = jnp.arange(other_cells, dtype=jnp.int32)
    near_pos = near_range // JW * KB + near_range % JW
    far_pos = far_range // (KB - JW) * KB + JW + far_range % (KB - JW)
    tile_keys = jax.random.split(keys_all[3], tile_total)

    def one_tile(tile_key, win_count, all_count):
        first_key, second_key = jax.random.split(tile_key)
        near_order = jax.random.permutation(first_key, window_cells)
        far_order = jax.random.permutation(second_key, other_cells)
        candidates = jnp.concatenate([near_pos[near_order], far_pos[far_order]])
        rank_keys = jnp.concatenate([jnp.where(near_range < win_count, 0, 2), jnp.where(far_range < all_count - win_count, 1, 2)])
        arranged = jnp.argsort(rank_keys, stable=True)
        return candidates[arranged][:CAPX].astype(jnp.int32)
    x_slots = jax.vmap(one_tile)(tile_keys, window_total, x_total)
    s_total = jax.random.randint(keys_all[4], (tile_total,), 1, CAPS + 1)
    s_total = s_total.at[jax.random.randint(keys_all[5], (), 0, tile_total)].set(CAPS)
    s_keys = jax.random.split(keys_all[6], tile_total)

    def one_mask(mask_key):
        return jax.random.permutation(mask_key, window_cells)[:CAPS].astype(jnp.int32)
    s_slots = jax.vmap(one_mask)(s_keys)
    return (x_slots.reshape(N_ROW, N_COL, CAPX), x_total.astype(jnp.int32).reshape(N_ROW, N_COL), s_slots.reshape(N_ROW, N_COL, CAPS), s_total.astype(jnp.int32).reshape(N_ROW, N_COL))


def draw_x_slots(key, part):
    return tile_layout(key)[0]


def draw_x_count(key, part):
    return tile_layout(key)[1]


def draw_s_slots(key, part):
    return tile_layout(key)[2]


def draw_s_count(key, part):
    return tile_layout(key)[3]


def block_levels(stream_key, dims, pieces, smallest, top_value):
    factor_of = 1.0
    for dim, blocks in pieces:
        draws = jax.random.uniform(jax.random.fold_in(jax.random.fold_in(stream_key, 6), dim), (blocks,), jnp.float32, smallest / len(pieces), top_value / len(pieces))
        factor_of = factor_of * jnp.repeat(jnp.exp(draws), dims[dim] // blocks).reshape((-1,) + (1,) * (len(dims) - 1 - dim))
    return factor_of


def noise(own_key, dims, deviation, reach, pieces=(), held_as=jnp.bfloat16):
    array = deviation * jax.random.normal(own_key, dims, jnp.float32)
    if pieces:
        array = array * block_levels(own_key, dims, pieces, -0.22, 0.18)
    return jnp.clip(array, -reach, reach).astype(held_as)


def setup_inputs(seed: int = 0) -> dict:
    key_list = jax.random.split(jax.random.key(seed), 6)
    x_blocks = noise(key_list[0], (N_ROW, N_COL, CAPX, BLOCK, BLOCK), 0.2, 1.1953125, ((0, 8), (1, 32)))
    x_slots = draw_x_slots(jax.random.fold_in(key_list[5], 71), 0)
    x_count = draw_x_count(jax.random.fold_in(key_list[5], 71), 0)
    s_slots = draw_s_slots(jax.random.fold_in(key_list[5], 71), 0)
    s_count = draw_s_count(jax.random.fold_in(key_list[5], 71), 0)
    return dict(x_blocks=x_blocks, x_slots=x_slots, x_count=x_count, s_slots=s_slots, s_count=s_count)


def place_sum(left_part, right_part, inner_col):
    products = jnp.einsum("nrxy,nyz->nrxz", left_part.astype(jnp.float32), right_part.astype(jnp.float32), precision=lax.Precision.HIGHEST)
    placing = (inner_col[:, None] == jnp.arange(JW, dtype=jnp.int32)[None, :]).astype(jnp.float32)
    return jnp.einsum("nj,nrxz->rjxz", placing, products, precision=lax.Precision.HIGHEST)


def reference(x_blocks, x_slots, x_count, s_slots, s_count):
    sentinel = N_ROW * N_COL * CAPX
    stacked = x_blocks.reshape(sentinel, BLOCK, BLOCK)
    padded = jnp.concatenate([stacked, jnp.zeros((1, BLOCK, BLOCK), stacked.dtype)], axis=0)
    ordinal = jnp.arange(CAPX, dtype=jnp.int32)
    slot_live = ordinal[None, None, :] < x_count[:, :, None]
    grid_row = jnp.arange(N_COL, dtype=jnp.int32)[None, :, None] * RB + x_slots // KB
    grid_col = jnp.arange(N_ROW, dtype=jnp.int32)[:, None, None] * KB + x_slots % KB
    grid_row = jnp.where(slot_live, grid_row, NB).astype(jnp.int32)
    grid_col = jnp.where(slot_live, grid_col, NB).astype(jnp.int32)
    slot_ids = jnp.arange(sentinel, dtype=jnp.int32).reshape(N_ROW, N_COL, CAPX)
    slot_table = jnp.full((NB + 1, NB + 1), sentinel, jnp.int32).at[grid_row, grid_col].set(slot_ids)
    col_ids = jnp.arange(N_COL, dtype=jnp.int32)[:, None]

    def multiply(col_id, right_vals, inner_row, inner_col, usable):
        row_lanes = col_id * RB + jnp.arange(RB, dtype=jnp.int32)
        picked = slot_table[row_lanes[None, :], inner_row[:, None]]
        left_part = padded[picked]
        right_part = jnp.where(usable[:, None, None], right_vals, jnp.zeros_like(right_vals))
        return place_sum(left_part, right_part, inner_col)

    def first_tile(tile_index):
        row_id = tile_index // N_COL
        col_id = tile_index % N_COL
        positions = x_slots[row_id][:, :CAPW]
        counts = x_count[row_id]
        inner_row = (col_ids * RB + positions // KB).reshape(-1)
        inner_col = (positions % KB).reshape(-1)
        usable = ((jnp.arange(CAPW, dtype=jnp.int32)[None, :] < counts[:, None]) & (positions % KB < JW)).reshape(-1)
        right_vals = x_blocks[row_id][:, :CAPW].reshape(N_COL * CAPW, BLOCK, BLOCK)
        product = multiply(col_id, right_vals, inner_row, inner_col, usable)
        own_slots = s_slots[row_id, col_id]
        own_live = jnp.arange(CAPS, dtype=jnp.int32) < s_count[row_id, col_id]
        chosen = product.reshape(RB * JW, BLOCK, BLOCK)[own_slots]
        return jnp.where(own_live[:, None, None], chosen, 0.0).astype(jnp.bfloat16)

    squares = lax.map(first_tile, jnp.arange(N_ROW * N_COL, dtype=jnp.int32))
    squares = squares.reshape(N_ROW, N_COL, CAPS, BLOCK, BLOCK)

    def second_tile(tile_index):
        row_id = tile_index // N_COL
        col_id = tile_index % N_COL
        positions = s_slots[row_id]
        counts = s_count[row_id]
        inner_row = (col_ids * RB + positions // JW).reshape(-1)
        inner_col = (positions % JW).reshape(-1)
        usable = (jnp.arange(CAPS, dtype=jnp.int32)[None, :] < counts[:, None]).reshape(-1)
        right_vals = squares[row_id].reshape(N_COL * CAPS, BLOCK, BLOCK)
        product = multiply(col_id, right_vals, inner_row, inner_col, usable)
        own_slots = s_slots[row_id, col_id]
        own_live = jnp.arange(CAPS, dtype=jnp.int32) < s_count[row_id, col_id]
        own_block = padded[slot_table[col_id * RB + own_slots // JW, row_id * KB + own_slots % JW]].astype(jnp.float32)
        combined = 1.5 * own_block - 0.5 * product.reshape(RB * JW, BLOCK, BLOCK)[own_slots]
        return jnp.where(own_live[:, None, None], combined, 0.0).astype(jnp.bfloat16)

    results = lax.map(second_tile, jnp.arange(N_ROW * N_COL, dtype=jnp.int32))
    results = results.reshape(N_ROW, N_COL, CAPS, BLOCK, BLOCK)
    return squares, results
```

```python
import jax
import jax.numpy as jnp
from jax import lax
from jax.experimental import pallas as pl
from jax.experimental.pallas import tpu as pltpu
from jax.sharding import PartitionSpec as P

RB = 8
JW = 2
KB = 32
NY, NX, NZ = 4, 4, 8
CAPX = 42
TAB = 2 * 8 * 4 * 4
MESH = pl.DeviceIdType.MESH
F32 = jnp.float32
BF16 = jnp.bfloat16


def spread(core, z):
    half = z // 4
    z2 = z % 4
    e = (core + half) % 2
    dz = (1 - e) * (z2 // 2 * 2 - 1) + e * (((z2 + 1) // 2 - 1) * 2)
    return half, (z + dz + NZ) % NZ


def unspread(core, zl):
    w = (zl - 4 * core + NZ) % NZ
    z2 = (w // 2 + 1) % 4
    e = (w + 1) // 2 % 2
    return (core + e) % 2, z2


def kernel(
    tab, x_hbm, sq_ref, out_ref,
    xs, g, acc, sown, dsend, drecv, ysend, yrecv,
    xsem, s1s, s1r, zs, zr, ds, dr, ys, yr,
):
    me_r = lax.axis_index("row")
    me_c = lax.axis_index("col")
    y, k = me_r // 2, me_r % 2
    x, z = me_c // NZ, me_c % NZ
    half, zland = spread(k, z)
    kin, z2in = unspread(k, z)

    x_copy = pltpu.make_async_copy(x_hbm, xs.at[pl.ds(0, CAPX)], xsem)
    x_copy.start()

    targets = [(2 * x + half, xt * NZ + zland) for xt in range(NX)]
    sources = [(2 * yt + kin, y * NZ + 4 * k + z2in) for yt in range(NY)]
    zplus = (me_r, x * NZ + (z + 1) % NZ)
    zminus = (me_r, x * NZ + (z + NZ - 1) % NZ)
    partner = (2 * y + 1 - k, me_c)
    ypeers = [(2 * ((y + d) % NY) + k, me_c) for d in range(1, NY)]

    barrier = pltpu.get_barrier_semaphore()
    everyone = targets + sources + [zplus, zminus, partner] + ypeers
    for peer in everyone:
        pl.semaphore_signal(barrier, inc=1, device_id=peer, device_id_type=MESH)

    xs[CAPX] = jnp.zeros((128, 128), BF16)
    pl.semaphore_wait(barrier, len(everyone))

    pending = []

    def send(src, dst, ssem, rsem, peer):
        copy = pltpu.make_async_remote_copy(
            src_ref=src, dst_ref=dst, send_sem=ssem, recv_sem=rsem,
            device_id=peer, device_id_type=MESH,
        )
        copy.start()
        pending.append(copy)

    def got(dst, ssem, rsem, peer):
        pltpu.make_async_remote_copy(
            src_ref=dst, dst_ref=dst, send_sem=ssem, recv_sem=rsem,
            device_id=peer, device_id_type=MESH,
        ).wait_recv()

    def phase(ph, own_src):
        for xt in range(NX):
            send(own_src, g.at[ph, zland, y], s1s.at[ph, xt], s1r.at[ph, y], targets[xt])
        for r in range(8):
            acc[r] = jnp.zeros((256, 128), F32)

        def forward(step, way, yi):
            group = (z + NZ - step) % NZ if way == 0 else (z + step) % NZ
            part = g.at[ph, group, yi]
            send(part, part, zs.at[ph, way, step, yi], zr.at[ph, way, step, yi], zplus if way == 0 else zminus)

        def ring_got(step, way, yi):
            group = (z + 2 * NZ - step - 1) % NZ if way == 0 else (z + step + 1) % NZ
            got(g.at[ph, group, yi], zs.at[ph, way, step, yi], zr.at[ph, way, step, yi], zplus if way == 0 else zminus)

        def multiply(zl):
            ksrc, z2 = unspread(k, zl)

            def one(yi, carry):
                r = 2 * yi + ksrc
                base = ((ph * 8 + r) * 4 + z2) * 4
                b = [xs[tab[base + i]] for i in range(4)]
                left = jnp.concatenate(
                    [jnp.concatenate([b[0], b[1]], axis=1), jnp.concatenate([b[2], b[3]], axis=1)], axis=0
                )
                right = g[ph, zl, yi].reshape(256, 128)
                acc[r] += jnp.dot(left, right, preferred_element_type=F32)
                return carry

            lax.fori_loop(0, NY, one, 0)

        for yi in range(NY):
            got(g.at[ph, z, yi], s1s.at[ph, 0], s1r.at[ph, yi], targets[0])
            forward(0, 0, yi)
            forward(0, 1, yi)
        if ph == 0:
            x_copy.wait()
        multiply(z)
        for step in range(4):
            for yi in range(NY):
                if step < 3:
                    ring_got(step, 0, yi)
                    if step + 1 < 3 or yi < 2:
                        forward(step + 1, 0, yi)
                    ring_got(step, 1, yi)
                    if step + 1 < 3 or yi >= 2:
                        forward(step + 1, 1, yi)
                else:
                    ring_got(step, 0 if yi < 2 else 1, yi)
            multiply((z + NZ - step - 1) % NZ)
            if step < 3:
                multiply((z + step + 1) % NZ)

        for yi in range(NY):
            dsend[ph, yi] = acc[2 * yi + 1 - k].astype(BF16)
        send(dsend.at[ph], drecv.at[ph], ds.at[ph], dr.at[ph], partner)
        got(drecv.at[ph], ds.at[ph], dr.at[ph], partner)
        for d in range(1, NY):
            yt = (y + d) % NY
            ysend[ph, d - 1] = (acc[2 * yt + k] + drecv[ph, yt].astype(F32)).astype(BF16)
            send(ysend.at[ph, d - 1], yrecv.at[ph, d - 1], ys.at[ph, d - 1], yr.at[ph, d - 1], ypeers[d - 1])
        total = acc[2 * y + k] + drecv[ph, y].astype(F32)
        for d in range(1, NY):
            got(yrecv.at[ph, d - 1], ys.at[ph, d - 1], yr.at[ph, d - 1], ypeers[d - 1])
            total = total + yrecv[ph, d - 1].astype(F32)
        return total.reshape(2, 128, 128)

    count = tab[TAB + 2]
    square = phase(0, x_hbm.at[pl.ds(0, 2)])
    for t in range(2):
        block = jnp.where(count > t, square[t], 0.0).astype(BF16)
        sown[t] = block
        sq_ref[t] = block
    second = phase(1, sown)
    for t in range(2):
        mixed = 1.5 * xs[tab[TAB + t]].astype(F32) - 0.5 * second[t]
        out_ref[t] = jnp.where(count > t, mixed, 0.0).astype(BF16)
    for copy in pending:
        copy.wait_send()


def local(x_blocks, x_slots, x_count, s_slots, s_count):
    row = lax.axis_index("row")
    col = lax.axis_index("col")
    ordinal = jnp.arange(CAPX, dtype=jnp.int32)
    own = lax.dynamic_slice(x_slots, (row, col, 0), (1, 1, CAPX)).reshape(CAPX)
    own_count = lax.dynamic_slice(x_count, (row, col), (1, 1)).reshape(())
    own = jnp.where(ordinal < own_count, own, -2)
    so = lax.dynamic_slice(s_slots, (0, col, 0), (8, 1, 2))[:, None, 0, :, None]
    lane = jnp.arange(2, dtype=jnp.int32)
    z2 = jnp.arange(4, dtype=jnp.int32)[None, :, None, None]

    def wanted(slots, count, stride):
        at = lax.dynamic_slice(slots, (0, 4 * row, 0), (8, 4, 2))[:, :, None, :]
        live = lane < lax.dynamic_slice(count, (0, 4 * row), (8, 4))[:, :, None, None]
        ok = live & (at % stride == so % JW)
        return jnp.where(ok, so // JW * KB + z2 * RB + at // stride, -1).reshape(-1)

    mine = lax.dynamic_slice(s_slots, (row, col, 0), (1, 1, 2)).reshape(2)
    targets = jnp.concatenate(
        [wanted(x_slots, x_count, KB), wanted(s_slots, s_count, JW), mine // JW * KB + mine % JW]
    )
    found = CAPX + jnp.sum(jnp.where(targets[:, None] == own, ordinal - CAPX, 0), axis=1)
    count = lax.dynamic_slice(s_count, (row, col), (1, 1)).reshape(1)
    tab = jnp.concatenate([found, count])
    dma = pltpu.SemaphoreType.DMA
    part = jax.ShapeDtypeStruct((2, 128, 128), BF16)
    vmem = pl.BlockSpec(memory_space=pltpu.VMEM)
    square, result = pl.pallas_call(
        kernel,
        out_shape=(part, part),
        in_specs=[pl.BlockSpec(memory_space=pltpu.SMEM), pl.BlockSpec(memory_space=pl.ANY)],
        out_specs=(vmem, vmem),
        scratch_shapes=[
            pltpu.VMEM((CAPX + 1, 128, 128), BF16),
            pltpu.VMEM((2, NZ, NY, 2, 128, 128), BF16),
            pltpu.VMEM((8, 256, 128), F32),
            pltpu.VMEM((2, 128, 128), BF16),
            pltpu.VMEM((2, NY, 256, 128), BF16),
            pltpu.VMEM((2, NY, 256, 128), BF16),
            pltpu.VMEM((2, NY - 1, 256, 128), BF16),
            pltpu.VMEM((2, NY - 1, 256, 128), BF16),
            dma,
            dma((2, NX)), dma((2, NY)),
            dma((2, 2, 4, NY)), dma((2, 2, 4, NY)),
            dma((2,)), dma((2,)),
            dma((2, NY - 1)), dma((2, NY - 1)),
        ],
        compiler_params=pltpu.CompilerParams(collective_id=0, has_side_effects=True),
    )(tab, x_blocks.reshape(CAPX, 128, 128))
    return square[None, None], result[None, None]


def solution(mesh):
    in_specs = (P("row", "col", None, None, None), P(), P(), P(), P())
    out_specs = (P("row", "col", None, None, None), P("row", "col", None, None, None))
    return jax.shard_map(local, mesh=mesh, in_specs=in_specs, out_specs=out_specs, check_vma=False)
```

```python
import jax
import jax.numpy as jnp
from jax import lax
from jax.experimental import pallas as pl
from jax.experimental.pallas import tpu as pltpu
from jax.sharding import PartitionSpec as P

RB = 8
JW = 2
KB = 32
NY, NX, NZ = 4, 4, 8
CAPX = 42
MESH = pl.DeviceIdType.MESH
F32 = jnp.float32
BF16 = jnp.bfloat16
I32 = jnp.int32


def spread(core, z):
    half = z // 4
    z2 = z % 4
    e = (core + half) % 2
    dz = (1 - e) * (z2 // 2 * 2 - 1) + e * (((z2 + 1) // 2 - 1) * 2)
    return half, (z + dz + NZ) % NZ


def unspread(core, zl):
    w = (zl - 4 * core + NZ) % NZ
    z2 = (w // 2 + 1) % 4
    e = (w + 1) // 2 % 2
    return (core + e) % 2, z2


def find_blocks(me_r, me_c, x_slots, x_count, s_slots, s_count, tabv):
    lane = lax.broadcasted_iota(I32, (8, 128), 1)
    lane32 = lax.broadcasted_iota(I32, (8, 32), 1)

    def column(values, at):
        return jnp.sum(jnp.where(lane32 == at, values, 0), axis=1, keepdims=True)

    rows = [s_slots[:, t, :] for t in range(2)]
    xc, sc = x_count[...], s_count[...]
    so = [column(rows[t], me_c) for t in range(2)]
    bit = lane // 2 % 2
    so_lane = jnp.where(bit == 0, so[0], so[1])
    at_row = jnp.zeros((8, 128), I32)
    at_col = jnp.zeros((8, 128), I32)
    live = jnp.zeros((8, 128), I32)
    for z2 in range(4):
        c = 4 * me_r + z2
        near = x_slots[:, c, :]
        counts = (column(xc, c), column(sc, c))
        for n in range(2):
            px = near[:, n : n + 1]
            ps = column(rows[n], c)
            for ph, p, stride in ((0, px, KB), (1, ps, JW)):
                here = (lane // 4 == ph * 4 + z2) & (lane % 2 == n)
                at_row = jnp.where(here, z2 * RB + p // stride, at_row)
                at_col = jnp.where(here, p % stride, at_col)
                live = jnp.where(here, jnp.where(counts[ph] > n, 1, 0), live)
    want = jnp.where((live == 1) & (at_col == so_lane % JW), so_lane // JW * KB + at_row, -1)
    for t in range(2):
        want = jnp.where(lane == 32 + t, so[t] // JW * KB + so[t] % JW, want)
    own = x_slots[me_r, pl.ds(me_c, 1), :]
    own_count = jnp.sum(jnp.where(lane32[:1] == me_c, x_count[pl.ds(me_r, 1), :], 0), axis=1, keepdims=True)
    own = jnp.where(lax.broadcasted_iota(I32, (1, CAPX), 1) < own_count, own, -2)
    found = jnp.full((8, 128), CAPX, I32)
    for s in range(CAPX):
        found = jnp.where(want == own[:, s : s + 1], s, found)
    tabv[...] = jnp.where(lane == 34, column(sc, me_c), found)


def kernel(
    x_slots, x_count, s_slots, s_count, x_hbm, out_ref,
    xs, g, acc, sown, drecv, ysend, yrecv, tabv, tab,
    xsem, tsem, as_, ar, bs, br, zas, zar, zbs, zbr, xbs, xbr, ds, dr, ys, yr,
):
    me_r = lax.axis_index("row")
    me_c = lax.axis_index("col")
    y, k = me_r // 2, me_r % 2
    x, z = me_c // NZ, me_c % NZ
    half, zland = spread(k, z)
    kin, z2in = unspread(k, z)

    x_copy = pltpu.make_async_copy(x_hbm, xs.at[pl.ds(0, CAPX)], xsem)
    x_copy.start()

    targets = [(2 * x + half, xt * NZ + zland) for xt in range(NX)]
    landing = (2 * x + half, y * NZ + zland)
    sources = [(2 * yt + kin, y * NZ + 4 * k + z2in) for yt in range(NY)]
    zpeer = [(me_r, x * NZ + (z + 1) % NZ), (me_r, x * NZ + (z + NZ - 1) % NZ)]
    partner = (2 * y + 1 - k, me_c)
    ypeer = [(2 * ((y + d) % NY) + k, me_c) for d in range(1, NY)]

    def xpeer(dx):
        return (me_r, (x + dx + NX) % NX * NZ + z)

    barrier = pltpu.get_barrier_semaphore()
    everyone = targets + sources + zpeer + [partner] + ypeer + [xpeer(1), xpeer(-1)]
    for peer in everyone:
        pl.semaphore_signal(barrier, inc=1, device_id=peer, device_id_type=MESH)
    xs[CAPX] = jnp.zeros((128, 128), BF16)
    pl.semaphore_wait(barrier, len(everyone))

    pending = []

    def remote(src, dst, sems, peer):
        return pltpu.make_async_remote_copy(
            src_ref=src, dst_ref=dst, send_sem=sems[0], recv_sem=sems[1],
            device_id=peer, device_id_type=MESH,
        )

    def send(src, dst, sems, peer):
        copy = remote(src, dst, sems, peer)
        copy.start()
        pending.append(copy)

    def got(dst, sems, peer):
        remote(dst, dst, sems, peer).wait_recv()

    def phase(ph, own_a, own_b):
        def block(zl, yi, n):
            return g.at[ph, zl, yi, n]

        send(own_b, block(zland, y, 1), (bs.at[ph], br.at[ph]), landing)
        for d in range(NX):
            xt = (x + d + 1) % NX
            peer = (2 * x + half, xt * NZ + zland)
            send(own_a, block(zland, y, 0), (as_.at[ph, d], ar.at[ph, y]), peer)

        if ph == 0:
            find_blocks(me_r, me_c, x_slots, x_count, s_slots, s_count, tabv)
            tab_copy = pltpu.make_async_copy(tabv, tab, tsem)
            tab_copy.start()
        for r in range(8):
            acc[ph, r] = jnp.zeros((256, 128), F32)
        if ph == 0:
            tab_copy.wait()
            x_copy.wait()

        def sign(zl):
            return 1 - 2 * (zl % 2)

        def xsems(slot, zl):
            return (xbs.at[ph, slot, zl], xbr.at[ph, slot, zl])

        def group(step, way):
            return (z + NZ - step) % NZ if way == 0 else (z + step) % NZ

        def ring(step, way, yi):
            zl = group(step, way)
            send(block(zl, yi, 0), block(zl, yi, 0), (zas.at[ph, way, step, yi], zar.at[ph, way, step, yi]), zpeer[way])

        def ring_got(step, way, yi):
            got(block(group(step + 1, way), yi, 0), (zas.at[ph, way, step, yi], zar.at[ph, way, step, yi]), zpeer[way])

        def ring_b(step, way):
            zl = group(step, way)
            send(block(zl, x, 1), block(zl, x, 1), (zbs.at[ph, way, step], zbr.at[ph, way, step]), zpeer[way])

        def ring_b_got(step, way):
            got(block(group(step + 1, way), x, 1), (zbs.at[ph, way, step], zbr.at[ph, way, step]), zpeer[way])

        def cast(zl):
            for slot, dx in ((0, sign(zl)), (1, -sign(zl))):
                send(block(zl, x, 1), block(zl, x, 1), xsems(slot, zl), xpeer(dx))

        def relay(zl):
            part = block(zl, (x - sign(zl) + NX) % NX, 1)
            got(part, xsems(0, zl), xpeer(1))
            send(part, part, xsems(2, zl), xpeer(sign(zl)))

        def multiply(zl):
            got(block(zl, (x + sign(zl) + NX) % NX, 1), xsems(1, zl), xpeer(1))
            got(block(zl, (x + 2) % NX, 1), xsems(2, zl), xpeer(1))
            ksrc, z2 = unspread(k, zl)

            def one(yi, carry):
                r = 2 * yi + ksrc
                base = (ph * 4 + z2) * 4
                b = [xs[tab[r, base + i]] for i in range(4)]
                left = jnp.concatenate(
                    [jnp.concatenate([b[0], b[1]], axis=1), jnp.concatenate([b[2], b[3]], axis=1)], axis=0
                )
                right = g[ph, zl, yi].reshape(256, 128)
                acc[ph, r] += jnp.dot(left, right, preferred_element_type=F32)
                return carry

            lax.fori_loop(0, NY, one, 0)

        got(block(z, x, 1), (bs.at[ph], br.at[ph]), partner)
        ring_b(0, 0)
        ring_b(0, 1)
        cast(z)
        for yi in range(NY):
            got(block(z, yi, 0), (as_.at[ph, 0], ar.at[ph, yi]), partner)
            ring(0, 0, yi)
            ring(0, 1, yi)
        arrived = [[z]] + [[group(s, 0), group(s, 1)] for s in range(1, 4)] + [[group(4, 0)]]
        for step in range(4):
            last = step == 3
            for way in range(1 if last else 2):
                ring_b_got(step, way)
                if step < 2 or (step == 2 and way == 0):
                    ring_b(step + 1, way)
                cast(group(step + 1, way))
            for zl in arrived[step]:
                relay(zl)
            for yi in range(NY):
                for way in range(2):
                    if last and way != yi // 2:
                        continue
                    ring_got(step, way, yi)
                    if step < 2 or (step == 2 and way == yi // 2):
                        ring(step + 1, way, yi)
            if step >= 1:
                for zl in arrived[step - 1]:
                    multiply(zl)
        for zl in arrived[4]:
            relay(zl)
        for zl in arrived[3] + arrived[4]:
            multiply(zl)

        for yi in range(NY):
            send(acc.at[ph, 2 * yi + 1 - k], drecv.at[ph, yi], (ds.at[ph, yi], dr.at[ph, yi]), partner)
        for yi in range(NY):
            got(drecv.at[ph, yi], (ds.at[ph, yi], dr.at[ph, yi]), partner)
        for d in (2, 1, 3):
            yt = (y + d) % NY
            ysend[ph, d - 1] = (acc[ph, 2 * yt + k] + drecv[ph, yt]).astype(BF16)
            send(ysend.at[ph, d - 1], yrecv.at[ph, d - 1], (ys.at[ph, d - 1], yr.at[ph, d - 1]), ypeer[d - 1])
        total = acc[ph, 2 * y + k] + drecv[ph, y]
        for d in (1, 3, 2):
            got(yrecv.at[ph, d - 1], (ys.at[ph, d - 1], yr.at[ph, d - 1]), ypeer[d - 1])
            total = total + yrecv[ph, d - 1].astype(F32)
        return total.reshape(2, 128, 128)

    square = phase(0, x_hbm.at[0], x_hbm.at[1])
    count = tab[me_r, 34]
    for t in range(2):
        block = jnp.where(count > t, square[t], 0.0).astype(BF16)
        sown[t] = block
        out_ref[t] = block
    second = phase(1, sown.at[0], sown.at[1])
    for t in range(2):
        mixed = 1.5 * xs[tab[me_r, 32 + t]].astype(F32) - 0.5 * second[t]
        out_ref[2 + t] = jnp.where(count > t, mixed, 0.0).astype(BF16)
    for copy in pending:
        copy.wait_send()


def split(both, square, result):
    square[...] = both[:2]
    result[...] = both[2:]


def local(x_blocks, x_slots, x_count, s_slots, s_count):
    dma = pltpu.SemaphoreType.DMA
    vmem = pl.BlockSpec(memory_space=pltpu.VMEM)
    both = pl.pallas_call(
        kernel,
        out_shape=jax.ShapeDtypeStruct((4, 128, 128), BF16),
        in_specs=[vmem] * 4 + [pl.BlockSpec(memory_space=pl.ANY)],
        out_specs=vmem,
        scratch_shapes=[
            pltpu.VMEM((CAPX + 1, 128, 128), BF16),
            pltpu.VMEM((2, NZ, NY, 2, 128, 128), BF16),
            pltpu.VMEM((2, 8, 256, 128), F32),
            pltpu.VMEM((2, 128, 128), BF16),
            pltpu.VMEM((2, NY, 256, 128), F32),
            pltpu.VMEM((2, NY - 1, 256, 128), BF16),
            pltpu.VMEM((2, NY - 1, 256, 128), BF16),
            pltpu.VMEM((8, 128), I32),
            pltpu.SMEM((8, 128), I32),
            dma, dma,
            dma((2, NX)), dma((2, NY)),
            dma((2,)), dma((2,)),
            dma((2, 2, 4, NY)), dma((2, 2, 4, NY)),
            dma((2, 2, 4)), dma((2, 2, 4)),
            dma((2, 3, NZ)), dma((2, 3, NZ)),
            dma((2, NY)), dma((2, NY)),
            dma((2, NY - 1)), dma((2, NY - 1)),
        ],
        compiler_params=pltpu.CompilerParams(collective_id=0, has_side_effects=True),
    )(x_slots, x_count, s_slots.transpose(0, 2, 1), s_count, x_blocks.reshape(CAPX, 128, 128))
    part = jax.ShapeDtypeStruct((2, 128, 128), BF16)
    square, result = pl.pallas_call(
        split, out_shape=(part, part), in_specs=[vmem], out_specs=(vmem, vmem)
    )(both)
    return square[None, None], result[None, None]


def solution(mesh):
    in_specs = (P("row", "col", None, None, None), P(), P(), P(), P())
    out_specs = (P("row", "col", None, None, None), P("row", "col", None, None, None))
    return jax.shard_map(local, mesh=mesh, in_specs=in_specs, out_specs=out_specs, check_vma=False)
```

```python
import jax
import jax.numpy as jnp
from jax import lax
from jax.experimental import pallas as pl
from jax.experimental.pallas import tpu as pltpu
from jax.sharding import PartitionSpec as P

RB = 8
JW = 2
KB = 32
NY, NX, NZ = 4, 4, 8
CAPX = 42
MESH = pl.DeviceIdType.MESH
F32 = jnp.float32
BF16 = jnp.bfloat16
I32 = jnp.int32


def spread(core, z):
    half = z // 4
    z2 = z % 4
    e = (core + half) % 2
    dz = (1 - e) * (z2 // 2 * 2 - 1) + e * (((z2 + 1) // 2 - 1) * 2)
    return half, (z + dz + NZ) % NZ


def unspread(core, zl):
    w = (zl - 4 * core + NZ) % NZ
    z2 = (w // 2 + 1) % 4
    e = (w + 1) // 2 % 2
    return (core + e) % 2, z2


def find_blocks(me_r, me_c, x_slots, x_count, s_slots, s_count, tabv):
    lane = lax.broadcasted_iota(I32, (8, 128), 1)
    lane32 = lax.broadcasted_iota(I32, (8, 32), 1)

    def column(values, at):
        return jnp.sum(jnp.where(lane32 == at, values, 0), axis=1, keepdims=True)

    rows = [s_slots[:, t, :] for t in range(2)]
    xc, sc = x_count[...], s_count[...]
    so = [column(rows[t], me_c) for t in range(2)]
    bit = lane // 2 % 2
    so_lane = jnp.where(bit == 0, so[0], so[1])
    at_row = jnp.zeros((8, 128), I32)
    at_col = jnp.zeros((8, 128), I32)
    live = jnp.zeros((8, 128), I32)
    for z2 in range(4):
        c = 4 * me_r + z2
        near = x_slots[:, c, :]
        counts = (column(xc, c), column(sc, c))
        for n in range(2):
            px = near[:, n : n + 1]
            ps = column(rows[n], c)
            for ph, p, stride in ((0, px, KB), (1, ps, JW)):
                here = (lane // 4 == ph * 4 + z2) & (lane % 2 == n)
                at_row = jnp.where(here, z2 * RB + p // stride, at_row)
                at_col = jnp.where(here, p % stride, at_col)
                live = jnp.where(here, jnp.where(counts[ph] > n, 1, 0), live)
    want = jnp.where((live == 1) & (at_col == so_lane % JW), so_lane // JW * KB + at_row, -1)
    for t in range(2):
        want = jnp.where(lane == 32 + t, so[t] // JW * KB + so[t] % JW, want)
    own = x_slots[me_r, pl.ds(me_c, 1), :]
    own_count = jnp.sum(jnp.where(lane32[:1] == me_c, x_count[pl.ds(me_r, 1), :], 0), axis=1, keepdims=True)
    own = jnp.where(lax.broadcasted_iota(I32, (1, CAPX), 1) < own_count, own, -2)
    found = jnp.full((8, 128), CAPX, I32)
    for s in range(CAPX):
        found = jnp.where(want == own[:, s : s + 1], s, found)
    tabv[...] = jnp.where(lane == 34, column(sc, me_c), found)


def kernel(
    x_slots_hbm, x_count_hbm, s_slots_hbm, s_count_hbm, x_hbm, out_ref,
    x_slots, x_count, s_slots, s_count, xs, g, acc, sown, drecv, ysend, yrecv, tabv, tab,
    xsem, tsem, isem, as_, ar, bs, br, zas, zar, zbs, zbr, xbs, xbr, ds, dr, ys, yr,
):
    me_r = lax.axis_index("row")
    me_c = lax.axis_index("col")
    y, k = me_r // 2, me_r % 2
    x, z = me_c // NZ, me_c % NZ
    half, zland = spread(k, z)
    kin, z2in = unspread(k, z)

    targets = [(2 * x + half, xt * NZ + zland) for xt in range(NX)]
    landing = (2 * x + half, y * NZ + zland)
    sources = [(2 * yt + kin, y * NZ + 4 * k + z2in) for yt in range(NY)]
    zpeer = [(me_r, x * NZ + (z + d + NZ) % NZ) for d in (1, -1, 2, -2)]
    partner = (2 * y + 1 - k, me_c)
    ypeer = [(2 * ((y + d) % NY) + k, me_c) for d in range(1, NY)]

    def xpeer(dx):
        return (me_r, (x + dx + NX) % NX * NZ + z)

    barrier = pltpu.get_barrier_semaphore()
    everyone = targets + sources + zpeer + [partner] + ypeer + [xpeer(1), xpeer(-1), xpeer(2)]
    for peer in everyone:
        pl.semaphore_signal(barrier, inc=1, device_id=peer, device_id_type=MESH)
    inputs = [
        pltpu.make_async_copy(a, b, isem.at[i])
        for i, (a, b) in enumerate(
            [(x_slots_hbm, x_slots), (x_count_hbm, x_count), (s_slots_hbm, s_slots), (s_count_hbm, s_count)]
        )
    ]
    x_copy = pltpu.make_async_copy(x_hbm, xs.at[pl.ds(0, CAPX)], xsem)
    for copy in inputs + [x_copy]:
        copy.start()
    xs[CAPX] = jnp.zeros((128, 128), BF16)
    pl.semaphore_wait(barrier, len(everyone))

    pending = []

    def remote(src, dst, sems, peer):
        return pltpu.make_async_remote_copy(
            src_ref=src, dst_ref=dst, send_sem=sems[0], recv_sem=sems[1],
            device_id=peer, device_id_type=MESH,
        )

    def send(src, dst, sems, peer):
        copy = remote(src, dst, sems, peer)
        copy.start()
        pending.append(copy)

    def got(dst, sems, peer):
        remote(dst, dst, sems, peer).wait_recv()

    def phase(ph, own_a, own_b):
        def block(zl, yi, n):
            return g.at[ph, zl, yi, n]

        send(own_b, block(zland, y, 1), (bs.at[ph], br.at[ph]), landing)
        for d in range(NX):
            xt = (x + d + 1) % NX
            peer = (2 * x + half, xt * NZ + zland)
            send(own_a, block(zland, y, 0), (as_.at[ph, d], ar.at[ph, y]), peer)

        if ph == 0:
            for copy in inputs:
                copy.wait()
            find_blocks(me_r, me_c, x_slots, x_count, s_slots, s_count, tabv)
            tab_copy = pltpu.make_async_copy(tabv, tab, tsem)
            tab_copy.start()
        for r in range(8):
            acc[ph, r] = jnp.zeros((256, 128), F32)
        if ph == 0:
            tab_copy.wait()
            x_copy.wait()

        def sign(zl):
            return 1 - 2 * (zl % 2)

        def xsems(slot, zl):
            return (xbs.at[ph, slot, zl], xbr.at[ph, slot, zl])

        def group(step, way):
            return (z + NZ - step) % NZ if way == 0 else (z + step) % NZ

        def ring(step, way, yi):
            zl = group(step, way)
            send(block(zl, yi, 0), block(zl, yi, 0), (zas.at[ph, way, step, yi], zar.at[ph, way, step, yi]), zpeer[way])

        def ring_got(step, way, yi):
            got(block(group(step + 1, way), yi, 0), (zas.at[ph, way, step, yi], zar.at[ph, way, step, yi]), zpeer[way])

        def send_b(zl, peer, at, rows=128, first=0):
            part = g.at[ph, zl, x, 1, pl.ds(first, rows)]
            send(part, part, (zbs.at[ph, at], zbr.at[ph, at]), zpeer[peer])

        def got_b(zl, at, rows=128, first=0):
            got(g.at[ph, zl, x, 1, pl.ds(first, rows)], (zbs.at[ph, at], zbr.at[ph, at]), zpeer[0])

        def cast(zl, direct=False):
            part = block(zl, x, 1)
            for slot, dx in ((2, 2), (0, sign(zl)), (1, -sign(zl))):
                if slot < 2 or direct:
                    send(part, part, xsems(slot, zl), xpeer(dx))

        def relay(zl):
            part = block(zl, (x - sign(zl) + NX) % NX, 1)
            got(part, xsems(0, zl), xpeer(1))
            send(part, part, xsems(2, zl), xpeer(sign(zl)))

        def multiply(zl, direct=False):
            if direct:
                got(block(zl, (x - sign(zl) + NX) % NX, 1), xsems(0, zl), xpeer(1))
            got(block(zl, (x + sign(zl) + NX) % NX, 1), xsems(1, zl), xpeer(1))
            got(block(zl, (x + 2) % NX, 1), xsems(2, zl), xpeer(1))
            ksrc, z2 = unspread(k, zl)

            def one(yi, carry):
                r = 2 * yi + ksrc
                base = (ph * 4 + z2) * 4
                b = [xs[tab[r, base + i]] for i in range(4)]
                left = jnp.concatenate(
                    [jnp.concatenate([b[0], b[1]], axis=1), jnp.concatenate([b[2], b[3]], axis=1)], axis=0
                )
                right = g[ph, zl, yi].reshape(256, 128)
                acc[ph, r] += jnp.dot(left, right, preferred_element_type=F32)
                return carry

            lax.fori_loop(0, NY, one, 0)

        def near(d):
            return (z + d + NZ) % NZ

        got(block(z, x, 1), (bs.at[ph], br.at[ph]), partner)
        for i, d in ((2, 2), (3, -2), (0, 1), (1, -1)):
            send_b(z, i, i)
        cast(z)
        for yi in range(NY):
            got(block(z, yi, 0), (as_.at[ph, 0], ar.at[ph, yi]), partner)
            ring(0, 0, yi)
            ring(0, 1, yi)
        for i, d in ((0, -1), (1, 1)):
            got_b(near(d), i)
            cast(near(d))
        for i, d in ((2, -2), (3, 2)):
            got_b(near(d), i)
            send_b(near(d), i - 2, 2 + i)
            send_b(near(d), i, 4 + i, 64, 64 * (i - 2))
            cast(near(d))
        relay(z)

        def advance(step):
            for yi in range(NY):
                for way in range(2):
                    if step == 3 and way != yi // 2:
                        continue
                    ring_got(step, way, yi)
                    if step < 2 or (step == 2 and way == yi // 2):
                        ring(step + 1, way, yi)

        advance(0)
        relay(near(1))
        relay(near(-1))
        for i, d in ((4, -3), (5, 3)):
            got_b(near(d), i)
            cast(near(d), True)
        got_b(near(4), 6, 64, 0)
        got_b(near(4), 7, 64, 64)
        cast(near(4), True)
        relay(near(2))
        relay(near(-2))
        advance(1)
        multiply(z)
        multiply(near(1))
        multiply(near(-1))
        advance(2)
        multiply(near(2))
        multiply(near(-2))
        multiply(near(3), True)
        multiply(near(-3), True)
        advance(3)
        multiply(near(4), True)

        order = [(y + d) % NY for d in (2, 1, 3, 0)]
        for yt in order:
            send(acc.at[ph, 2 * yt + 1 - k], drecv.at[ph, yt], (ds.at[ph, yt], dr.at[ph, yt]), partner)
        for d, yt in zip((2, 1, 3), order):
            got(drecv.at[ph, yt], (ds.at[ph, yt], dr.at[ph, yt]), partner)
            ysend[ph, d - 1] = (acc[ph, 2 * yt + k] + drecv[ph, yt]).astype(BF16)
            send(ysend.at[ph, d - 1], yrecv.at[ph, d - 1], (ys.at[ph, d - 1], yr.at[ph, d - 1]), ypeer[d - 1])
        got(drecv.at[ph, y], (ds.at[ph, y], dr.at[ph, y]), partner)
        total = acc[ph, 2 * y + k] + drecv[ph, y]
        for d in (1, 3, 2):
            got(yrecv.at[ph, d - 1], (ys.at[ph, d - 1], yr.at[ph, d - 1]), ypeer[d - 1])
            total = total + yrecv[ph, d - 1].astype(F32)
        return total.reshape(2, 128, 128)

    square = phase(0, x_hbm.at[0], x_hbm.at[1])
    count = tab[me_r, 34]
    for t in range(2):
        block = jnp.where(count > t, square[t], 0.0).astype(BF16)
        sown[t] = block
        out_ref[t] = block
    second = phase(1, sown.at[0], sown.at[1])
    for t in range(2):
        mixed = 1.5 * xs[tab[me_r, 32 + t]].astype(F32) - 0.5 * second[t]
        out_ref[2 + t] = jnp.where(count > t, mixed, 0.0).astype(BF16)
    for copy in pending:
        copy.wait_send()


def split(both, square, result):
    square[...] = both[:2]
    result[...] = both[2:]


def local(x_blocks, x_slots, x_count, s_slots, s_count):
    dma = pltpu.SemaphoreType.DMA
    vmem = pl.BlockSpec(memory_space=pltpu.VMEM)
    both = pl.pallas_call(
        kernel,
        out_shape=jax.ShapeDtypeStruct((4, 128, 128), BF16),
        in_specs=[pl.BlockSpec(memory_space=pl.ANY)] * 5,
        out_specs=vmem,
        scratch_shapes=[
            pltpu.VMEM((8, 32, CAPX), I32),
            pltpu.VMEM((8, 32), I32),
            pltpu.VMEM((8, 2, 32), I32),
            pltpu.VMEM((8, 32), I32),
            pltpu.VMEM((CAPX + 1, 128, 128), BF16),
            pltpu.VMEM((2, NZ, NY, 2, 128, 128), BF16),
            pltpu.VMEM((2, 8, 256, 128), F32),
            pltpu.VMEM((2, 128, 128), BF16),
            pltpu.VMEM((2, NY, 256, 128), F32),
            pltpu.VMEM((2, NY - 1, 256, 128), BF16),
            pltpu.VMEM((2, NY - 1, 256, 128), BF16),
            pltpu.VMEM((8, 128), I32),
            pltpu.SMEM((8, 128), I32),
            dma, dma, dma((4,)),
            dma((2, NX)), dma((2, NY)),
            dma((2,)), dma((2,)),
            dma((2, 2, 4, NY)), dma((2, 2, 4, NY)),
            dma((2, 8)), dma((2, 8)),
            dma((2, 3, NZ)), dma((2, 3, NZ)),
            dma((2, NY)), dma((2, NY)),
            dma((2, NY - 1)), dma((2, NY - 1)),
        ],
        compiler_params=pltpu.CompilerParams(collective_id=0, has_side_effects=True),
    )(x_slots, x_count, s_slots.transpose(0, 2, 1), s_count, x_blocks.reshape(CAPX, 128, 128))
    part = jax.ShapeDtypeStruct((2, 128, 128), BF16)
    square, result = pl.pallas_call(
        split, out_shape=(part, part), in_specs=[vmem], out_specs=(vmem, vmem)
    )(both)
    return square[None, None], result[None, None]


def solution(mesh):
    in_specs = (P("row", "col", None, None, None), P(), P(), P(), P())
    out_specs = (P("row", "col", None, None, None), P("row", "col", None, None, None))
    return jax.shard_map(local, mesh=mesh, in_specs=in_specs, out_specs=out_specs, check_vma=False)
```

```python
import jax
import jax.numpy as jnp
from jax import lax
from jax.experimental import pallas as pl
from jax.experimental.pallas import tpu as pltpu
from jax.sharding import PartitionSpec as P

RB = 8
JW = 2
KB = 32
NY, NX, NZ = 4, 4, 8
CAPX = 42
MESH = pl.DeviceIdType.MESH
F32 = jnp.float32
BF16 = jnp.bfloat16
I32 = jnp.int32


def spread(core, z):
    half = z // 4
    z2 = z % 4
    e = (core + half) % 2
    dz = (1 - e) * (z2 // 2 * 2 - 1) + e * (((z2 + 1) // 2 - 1) * 2)
    return half, (z + dz + NZ) % NZ


def unspread(core, zl):
    w = (zl - 4 * core + NZ) % NZ
    z2 = (w // 2 + 1) % 4
    e = (w + 1) // 2 % 2
    return (core + e) % 2, z2


def find_blocks(me_r, me_c, x_slots, x_count, s_slots, s_count, tabv):
    lane = lax.broadcasted_iota(I32, (8, 128), 1)
    lane32 = lax.broadcasted_iota(I32, (8, 32), 1)

    def column(values, at):
        return jnp.sum(jnp.where(lane32 == at, values, 0), axis=1, keepdims=True)

    rows = [s_slots[:, t, :] for t in range(2)]
    xc, sc = x_count[...], s_count[...]
    so = [column(rows[t], me_c) for t in range(2)]
    bit = lane // 2 % 2
    so_lane = jnp.where(bit == 0, so[0], so[1])
    at_row = jnp.zeros((8, 128), I32)
    at_col = jnp.zeros((8, 128), I32)
    live = jnp.zeros((8, 128), I32)
    for z2 in range(4):
        c = 4 * me_r + z2
        near = x_slots[:, c, :]
        counts = (column(xc, c), column(sc, c))
        for n in range(2):
            px = near[:, n : n + 1]
            ps = column(rows[n], c)
            for ph, p, stride in ((0, px, KB), (1, ps, JW)):
                here = (lane // 4 == ph * 4 + z2) & (lane % 2 == n)
                at_row = jnp.where(here, z2 * RB + p // stride, at_row)
                at_col = jnp.where(here, p % stride, at_col)
                live = jnp.where(here, jnp.where(counts[ph] > n, 1, 0), live)
    want = jnp.where((live == 1) & (at_col == so_lane % JW), so_lane // JW * KB + at_row, -1)
    for t in range(2):
        want = jnp.where(lane == 32 + t, so[t] // JW * KB + so[t] % JW, want)
    own = x_slots[me_r, pl.ds(me_c, 1), :]
    own_count = jnp.sum(jnp.where(lane32[:1] == me_c, x_count[pl.ds(me_r, 1), :], 0), axis=1, keepdims=True)
    own = jnp.where(lax.broadcasted_iota(I32, (1, CAPX), 1) < own_count, own, -2)
    found = jnp.full((8, 128), CAPX, I32)
    for s in range(CAPX):
        found = jnp.where(want == own[:, s : s + 1], s, found)
    tabv[...] = jnp.where(lane == 34, column(sc, me_c), found)


def kernel(
    x_slots_hbm, x_count_hbm, s_slots_hbm, s_count_hbm, x_hbm, out_ref,
    x_slots, x_count, s_slots, s_count, xs, g, acc, sown, drecv, ysend, yrecv, tabv, tab,
    xsem, tsem, isem, as_, ar, bs, br, zas, zar, zbs, zbr, xbs, xbr, ds, dr, ys, yr,
):
    me_r = lax.axis_index("row")
    me_c = lax.axis_index("col")
    y, k = me_r // 2, me_r % 2
    x, z = me_c // NZ, me_c % NZ
    half, zland = spread(k, z)
    kin, z2in = unspread(k, z)

    targets = [(2 * x + half, xt * NZ + zland) for xt in range(NX)]
    landing = (2 * x + half, y * NZ + zland)
    sources = [(2 * yt + kin, y * NZ + 4 * k + z2in) for yt in range(NY)]
    zpeer = [(me_r, x * NZ + (z + d + NZ) % NZ) for d in (1, -1, 2, -2)]
    partner = (2 * y + 1 - k, me_c)
    ypeer = [(2 * ((y + d) % NY) + k, me_c) for d in range(1, NY)]

    def xpeer(dx):
        return (me_r, (x + dx + NX) % NX * NZ + z)

    barrier = pltpu.get_barrier_semaphore()
    everyone = targets + sources + zpeer + [partner] + ypeer + [xpeer(1), xpeer(-1), xpeer(2)]
    for peer in everyone:
        pl.semaphore_signal(barrier, inc=1, device_id=peer, device_id_type=MESH)
    inputs = [
        pltpu.make_async_copy(a, b, isem.at[i])
        for i, (a, b) in enumerate(
            [(x_slots_hbm, x_slots), (x_count_hbm, x_count), (s_slots_hbm, s_slots), (s_count_hbm, s_count)]
        )
    ]
    x_copy = pltpu.make_async_copy(x_hbm, xs.at[pl.ds(0, CAPX)], xsem)
    for copy in inputs + [x_copy]:
        copy.start()
    xs[CAPX] = jnp.zeros((128, 128), BF16)
    pl.semaphore_wait(barrier, len(everyone))

    pending = []

    def remote(src, dst, sems, peer):
        return pltpu.make_async_remote_copy(
            src_ref=src, dst_ref=dst, send_sem=sems[0], recv_sem=sems[1],
            device_id=peer, device_id_type=MESH,
        )

    def send(src, dst, sems, peer):
        copy = remote(src, dst, sems, peer)
        copy.start()
        pending.append(copy)

    def got(dst, sems, peer):
        remote(dst, dst, sems, peer).wait_recv()

    def launch(ph, n, own):
        part = g.at[ph, zland, y, n]
        if n == 1:
            send(own, part, (bs.at[ph], br.at[ph]), landing)
            return
        for d in range(NX):
            peer = (2 * x + half, (x + d + 1) % NX * NZ + zland)
            send(own, part, (as_.at[ph, d], ar.at[ph, y]), peer)

    def phase(ph, finish):
        def block(zl, yi, n):
            return g.at[ph, zl, yi, n]

        if ph == 0:
            for copy in inputs:
                copy.wait()
            find_blocks(me_r, me_c, x_slots, x_count, s_slots, s_count, tabv)
            tab_copy = pltpu.make_async_copy(tabv, tab, tsem)
            tab_copy.start()
        for r in range(8):
            acc[ph, r] = jnp.zeros((256, 128), F32)
        if ph == 0:
            tab_copy.wait()
            x_copy.wait()

        def sign(zl):
            return 1 - 2 * (zl % 2)

        def xsems(slot, zl):
            return (xbs.at[ph, slot, zl], xbr.at[ph, slot, zl])

        def group(step, way):
            return (z + NZ - step) % NZ if way == 0 else (z + step) % NZ

        def ring(step, way, yi):
            zl = group(step, way)
            send(block(zl, yi, 0), block(zl, yi, 0), (zas.at[ph, way, step, yi], zar.at[ph, way, step, yi]), zpeer[way])

        def ring_got(step, way, yi):
            got(block(group(step + 1, way), yi, 0), (zas.at[ph, way, step, yi], zar.at[ph, way, step, yi]), zpeer[way])

        def send_b(zl, peer, at, rows=128, first=0):
            part = g.at[ph, zl, x, 1, pl.ds(first, rows)]
            send(part, part, (zbs.at[ph, at], zbr.at[ph, at]), zpeer[peer])

        def got_b(zl, at, rows=128, first=0):
            got(g.at[ph, zl, x, 1, pl.ds(first, rows)], (zbs.at[ph, at], zbr.at[ph, at]), zpeer[0])

        def cast(zl, direct=False):
            part = block(zl, x, 1)
            for slot, dx in ((2, 2), (0, sign(zl)), (1, -sign(zl))):
                if slot < 2 or direct:
                    send(part, part, xsems(slot, zl), xpeer(dx))

        def relay(zl):
            part = block(zl, (x - sign(zl) + NX) % NX, 1)
            got(part, xsems(0, zl), xpeer(1))
            send(part, part, xsems(2, zl), xpeer(sign(zl)))

        def multiply(zl, direct=False):
            if direct:
                got(block(zl, (x - sign(zl) + NX) % NX, 1), xsems(0, zl), xpeer(1))
            got(block(zl, (x + sign(zl) + NX) % NX, 1), xsems(1, zl), xpeer(1))
            got(block(zl, (x + 2) % NX, 1), xsems(2, zl), xpeer(1))
            ksrc, z2 = unspread(k, zl)

            def one(yi, carry):
                r = 2 * yi + ksrc
                base = (ph * 4 + z2) * 4
                b = [xs[tab[r, base + i]] for i in range(4)]
                left = jnp.concatenate(
                    [jnp.concatenate([b[0], b[1]], axis=1), jnp.concatenate([b[2], b[3]], axis=1)], axis=0
                )
                right = g[ph, zl, yi].reshape(256, 128)
                acc[ph, r] += jnp.dot(left, right, preferred_element_type=F32)
                return carry

            lax.fori_loop(0, NY, one, 0, unroll=True)

        def near(d):
            return (z + d + NZ) % NZ

        got(block(z, x, 1), (bs.at[ph], br.at[ph]), partner)
        for i, d in ((2, 2), (3, -2), (0, 1), (1, -1)):
            send_b(z, i, i)
        cast(z, True)
        for yi in range(NY):
            got(block(z, yi, 0), (as_.at[ph, 0], ar.at[ph, yi]), partner)
            ring(0, 0, yi)
            ring(0, 1, yi)
        for i, d in ((0, -1), (1, 1)):
            got_b(near(d), i)
            cast(near(d), True)
        for i, d in ((2, -2), (3, 2)):
            got_b(near(d), i)
            send_b(near(d), i - 2, 2 + i)
            send_b(near(d), i, 4 + i, 64, 64 * (i - 2))
            cast(near(d), True)

        def advance(step):
            for yi in range(NY):
                for way in range(2):
                    if step == 3 and way != yi // 2:
                        continue
                    ring_got(step, way, yi)
                    if step < 2 or (step == 2 and way == yi // 2):
                        ring(step + 1, way, yi)

        advance(0)
        for i, d in ((4, -3), (5, 3)):
            got_b(near(d), i)
            cast(near(d), True)
        got_b(near(4), 6, 64, 0)
        got_b(near(4), 7, 64, 64)
        cast(near(4), True)
        advance(1)
        multiply(z, True)
        multiply(near(1), True)
        multiply(near(-1), True)
        advance(2)
        multiply(near(2), True)
        multiply(near(-2), True)
        multiply(near(3), True)
        multiply(near(-3), True)
        advance(3)
        multiply(near(4), True)

        order = [(y + d) % NY for d in (2, 1, 3, 0)]
        for t in (1, 0):
            rows = pl.ds(128 * t, 128)
            for yt in order:
                send(acc.at[ph, 2 * yt + 1 - k, rows], drecv.at[ph, yt, rows], (ds.at[ph, t, yt], dr.at[ph, t, yt]), partner)

        def paired(t, yt):
            rows = pl.ds(128 * t, 128)
            got(drecv.at[ph, yt, rows], (ds.at[ph, t, yt], dr.at[ph, t, yt]), partner)
            return acc[ph, 2 * yt + k, rows] + drecv[ph, yt, rows]

        for t in (1, 0):
            for d, yt in zip((2, 1, 3), order):
                ysend[ph, t, d - 1] = paired(t, yt).astype(BF16)
                part = (ysend.at[ph, t, d - 1], yrecv.at[ph, t, d - 1])
                send(*part, (ys.at[ph, t, d - 1], yr.at[ph, t, d - 1]), ypeer[d - 1])
        for t in (1, 0):
            total = paired(t, y)
            for d in (1, 3, 2):
                got(yrecv.at[ph, t, d - 1], (ys.at[ph, t, d - 1], yr.at[ph, t, d - 1]), ypeer[d - 1])
                total = total + yrecv[ph, t, d - 1].astype(F32)
            finish(t, total)

    def squared(t, total):
        block = jnp.where(tab[me_r, 34] > t, total, 0.0).astype(BF16)
        sown[t] = block
        launch(1, t, sown.at[t])
        out_ref[t] = block

    def mixed(t, total):
        value = 1.5 * xs[tab[me_r, 32 + t]].astype(F32) - 0.5 * total
        out_ref[2 + t] = jnp.where(tab[me_r, 34] > t, value, 0.0).astype(BF16)

    launch(0, 1, x_hbm.at[1])
    launch(0, 0, x_hbm.at[0])
    phase(0, squared)
    phase(1, mixed)
    for copy in pending:
        copy.wait_send()


def split(both, square, result):
    square[...] = both[:2]
    result[...] = both[2:]


def local(x_blocks, x_slots, x_count, s_slots, s_count):
    dma = pltpu.SemaphoreType.DMA
    vmem = pl.BlockSpec(memory_space=pltpu.VMEM)
    both = pl.pallas_call(
        kernel,
        out_shape=jax.ShapeDtypeStruct((4, 128, 128), BF16),
        in_specs=[pl.BlockSpec(memory_space=pl.ANY)] * 5,
        out_specs=vmem,
        scratch_shapes=[
            pltpu.VMEM((8, 32, CAPX), I32),
            pltpu.VMEM((8, 32), I32),
            pltpu.VMEM((8, 2, 32), I32),
            pltpu.VMEM((8, 32), I32),
            pltpu.VMEM((CAPX + 1, 128, 128), BF16),
            pltpu.VMEM((2, NZ, NY, 2, 128, 128), BF16),
            pltpu.VMEM((2, 8, 256, 128), F32),
            pltpu.VMEM((2, 128, 128), BF16),
            pltpu.VMEM((2, NY, 256, 128), F32),
            pltpu.VMEM((2, 2, NY - 1, 128, 128), BF16),
            pltpu.VMEM((2, 2, NY - 1, 128, 128), BF16),
            pltpu.VMEM((8, 128), I32),
            pltpu.SMEM((8, 128), I32),
            dma, dma, dma((4,)),
            dma((2, NX)), dma((2, NY)),
            dma((2,)), dma((2,)),
            dma((2, 2, 4, NY)), dma((2, 2, 4, NY)),
            dma((2, 8)), dma((2, 8)),
            dma((2, 3, NZ)), dma((2, 3, NZ)),
            dma((2, 2, NY)), dma((2, 2, NY)),
            dma((2, 2, NY - 1)), dma((2, 2, NY - 1)),
        ],
        compiler_params=pltpu.CompilerParams(collective_id=0, has_side_effects=True),
    )(x_slots, x_count, s_slots.transpose(0, 2, 1), s_count, x_blocks.reshape(CAPX, 128, 128))
    part = jax.ShapeDtypeStruct((2, 128, 128), BF16)
    square, result = pl.pallas_call(
        split, out_shape=(part, part), in_specs=[vmem], out_specs=(vmem, vmem)
    )(both)
    return square[None, None], result[None, None]


def solution(mesh):
    in_specs = (P("row", "col", None, None, None), P(), P(), P(), P())
    out_specs = (P("row", "col", None, None, None), P("row", "col", None, None, None))
    return jax.shard_map(local, mesh=mesh, in_specs=in_specs, out_specs=out_specs, check_vma=False)
```

```python
import jax
import jax.numpy as jnp
from jax import lax
from jax.experimental import pallas as pl
from jax.experimental.pallas import tpu as pltpu
from jax.sharding import PartitionSpec as P

RB = 8
JW = 2
KB = 32
NY, NX, NZ = 4, 4, 8
CAPX = 42
MESH = pl.DeviceIdType.MESH
F32 = jnp.float32
BF16 = jnp.bfloat16
I32 = jnp.int32


def spread(core, z):
    half = z // 4
    z2 = z % 4
    e = (core + half) % 2
    dz = (1 - e) * (z2 // 2 * 2 - 1) + e * (((z2 + 1) // 2 - 1) * 2)
    return half, (z + dz + NZ) % NZ


def unspread(core, zl):
    w = (zl - 4 * core + NZ) % NZ
    z2 = (w // 2 + 1) % 4
    e = (w + 1) // 2 % 2
    return (core + e) % 2, z2


def find_blocks(me_r, me_c, x_slots, x_count, s_slots, s_count, tabv):
    lane = lax.broadcasted_iota(I32, (8, 128), 1)
    lane32 = lax.broadcasted_iota(I32, (8, 32), 1)

    def column(values, at):
        return jnp.sum(jnp.where(lane32 == at, values, 0), axis=1, keepdims=True)

    rows = [s_slots[:, t, :] for t in range(2)]
    xc, sc = x_count[...], s_count[...]
    so = [column(rows[t], me_c) for t in range(2)]
    bit = lane // 2 % 2
    so_lane = jnp.where(bit == 0, so[0], so[1])
    at_row = jnp.zeros((8, 128), I32)
    at_col = jnp.zeros((8, 128), I32)
    live = jnp.zeros((8, 128), I32)
    for z2 in range(4):
        c = 4 * me_r + z2
        near = x_slots[:, c, :]
        counts = (column(xc, c), column(sc, c))
        for n in range(2):
            px = near[:, n : n + 1]
            ps = column(rows[n], c)
            for ph, p, stride in ((0, px, KB), (1, ps, JW)):
                here = (lane // 4 == ph * 4 + z2) & (lane % 2 == n)
                at_row = jnp.where(here, z2 * RB + p // stride, at_row)
                at_col = jnp.where(here, p % stride, at_col)
                live = jnp.where(here, jnp.where(counts[ph] > n, 1, 0), live)
    want = jnp.where((live == 1) & (at_col == so_lane % JW), so_lane // JW * KB + at_row, -1)
    for t in range(2):
        want = jnp.where(lane == 32 + t, so[t] // JW * KB + so[t] % JW, want)
    own = x_slots[me_r, pl.ds(me_c, 1), :]
    own_count = jnp.sum(jnp.where(lane32[:1] == me_c, x_count[pl.ds(me_r, 1), :], 0), axis=1, keepdims=True)
    own = jnp.where(lax.broadcasted_iota(I32, (1, CAPX), 1) < own_count, own, -2)
    found = jnp.full((8, 128), CAPX, I32)
    for s in range(CAPX):
        found = jnp.where(want == own[:, s : s + 1], s, found)
    tabv[...] = jnp.where(lane == 34, column(sc, me_c), found)


def kernel(
    x_slots_hbm, x_count_hbm, s_slots_hbm, s_count_hbm, x_hbm, out_ref,
    x_slots, x_count, s_slots, s_count, xs, g, acc, sown, drecv, ysend, yrecv, tabv, tab,
    xsem, tsem, isem, as_, ar, bs, br, zas, zar, zbs, zbr, xbs, xbr, ds, dr, ys, yr,
):
    me_r = lax.axis_index("row")
    me_c = lax.axis_index("col")
    y, k = me_r // 2, me_r % 2
    x, z = me_c // NZ, me_c % NZ
    half, zland = spread(k, z)
    kin, z2in = unspread(k, z)

    targets = [(2 * x + half, xt * NZ + zland) for xt in range(NX)]
    landing = (2 * x + half, y * NZ + zland)
    sources = [(2 * yt + kin, y * NZ + 4 * k + z2in) for yt in range(NY)]
    zpeer = [(me_r, x * NZ + (z + d + NZ) % NZ) for d in (1, -1, 2, -2)]
    partner = (2 * y + 1 - k, me_c)
    ypeer = [(2 * ((y + d) % NY) + k, me_c) for d in range(1, NY)]

    def xpeer(dx):
        return (me_r, (x + dx + NX) % NX * NZ + z)

    barrier = pltpu.get_barrier_semaphore()
    everyone = targets + sources + zpeer + [partner] + ypeer + [xpeer(1), xpeer(-1), xpeer(2)]
    for peer in everyone:
        pl.semaphore_signal(barrier, inc=1, device_id=peer, device_id_type=MESH)
    inputs = [
        pltpu.make_async_copy(a, b, isem.at[i])
        for i, (a, b) in enumerate(
            [(x_slots_hbm, x_slots), (x_count_hbm, x_count), (s_slots_hbm, s_slots), (s_count_hbm, s_count)]
        )
    ]
    x_copy = pltpu.make_async_copy(x_hbm, xs.at[pl.ds(0, CAPX)], xsem)
    for copy in inputs + [x_copy]:
        copy.start()
    xs[CAPX] = jnp.zeros((128, 128), BF16)
    pl.semaphore_wait(barrier, len(everyone))

    pending = []

    def remote(src, dst, sems, peer):
        return pltpu.make_async_remote_copy(
            src_ref=src, dst_ref=dst, send_sem=sems[0], recv_sem=sems[1],
            device_id=peer, device_id_type=MESH,
        )

    def send(src, dst, sems, peer):
        copy = remote(src, dst, sems, peer)
        copy.start()
        pending.append(copy)

    def got(dst, sems, peer):
        remote(dst, dst, sems, peer).wait_recv()

    def launch(ph, n, own):
        part = g.at[ph, zland, y, n]
        if n == 1:
            send(own, part, (bs.at[ph], br.at[ph]), landing)
            return
        for d in range(NX):
            peer = (2 * x + half, (x + d + 1) % NX * NZ + zland)
            send(own, part, (as_.at[ph, d], ar.at[ph, y]), peer)

    def phase(ph, finish):
        def block(zl, yi, n):
            return g.at[ph, zl, yi, n]

        if ph == 0:
            for copy in inputs:
                copy.wait()
            find_blocks(me_r, me_c, x_slots, x_count, s_slots, s_count, tabv)
            tab_copy = pltpu.make_async_copy(tabv, tab, tsem)
            tab_copy.start()
        for r in range(8):
            acc[ph, r] = jnp.zeros((256, 128), F32)
        if ph == 0:
            tab_copy.wait()
            x_copy.wait()

        def sign(zl):
            return 1 - 2 * (zl % 2)

        def xsems(slot, zl):
            return (xbs.at[ph, slot, zl], xbr.at[ph, slot, zl])

        def group(step, way):
            return (z + NZ - step) % NZ if way == 0 else (z + step) % NZ

        def ring(step, way, yi):
            zl = group(step, way)
            send(block(zl, yi, 0), block(zl, yi, 0), (zas.at[ph, way, step, yi], zar.at[ph, way, step, yi]), zpeer[way])

        def ring_got(step, way, yi):
            got(block(group(step + 1, way), yi, 0), (zas.at[ph, way, step, yi], zar.at[ph, way, step, yi]), zpeer[way])

        def send_b(zl, peer, at, rows=128, first=0):
            part = g.at[ph, zl, x, 1, pl.ds(first, rows)]
            send(part, part, (zbs.at[ph, at], zbr.at[ph, at]), zpeer[peer])

        def got_b(zl, at, rows=128, first=0):
            got(g.at[ph, zl, x, 1, pl.ds(first, rows)], (zbs.at[ph, at], zbr.at[ph, at]), zpeer[0])

        def cast(zl, direct=False):
            part = block(zl, x, 1)
            for slot, dx in ((2, 2), (0, sign(zl)), (1, -sign(zl))):
                if slot < 2 or direct:
                    send(part, part, xsems(slot, zl), xpeer(dx))

        def relay(zl):
            part = block(zl, (x - sign(zl) + NX) % NX, 1)
            got(part, xsems(0, zl), xpeer(1))
            send(part, part, xsems(2, zl), xpeer(sign(zl)))

        def multiply(zl, direct=False):
            if direct:
                got(block(zl, (x - sign(zl) + NX) % NX, 1), xsems(0, zl), xpeer(1))
            got(block(zl, (x + sign(zl) + NX) % NX, 1), xsems(1, zl), xpeer(1))
            got(block(zl, (x + 2) % NX, 1), xsems(2, zl), xpeer(1))
            ksrc, z2 = unspread(k, zl)

            def one(yi, carry):
                r = 2 * yi + ksrc
                base = (ph * 4 + z2) * 4
                b = [xs[tab[r, base + i]] for i in range(4)]
                left = jnp.concatenate(
                    [jnp.concatenate([b[0], b[1]], axis=1), jnp.concatenate([b[2], b[3]], axis=1)], axis=0
                )
                right = g[ph, zl, yi].reshape(256, 128)
                acc[ph, r] += jnp.dot(left, right, preferred_element_type=F32)
                return carry

            lax.fori_loop(0, NY, one, 0, unroll=True)

        def near(d):
            return (z + d + NZ) % NZ

        got(block(z, x, 1), (bs.at[ph], br.at[ph]), partner)
        for i, d in ((2, 2), (3, -2), (0, 1), (1, -1)):
            send_b(z, i, i)
        cast(z, True)
        for yi in range(NY):
            got(block(z, yi, 0), (as_.at[ph, 0], ar.at[ph, yi]), partner)
            ring(0, 0, yi)
            ring(0, 1, yi)
        for i, d in ((0, -1), (1, 1)):
            got_b(near(d), i)
            cast(near(d), True)
        for i, d in ((2, -2), (3, 2)):
            got_b(near(d), i)
            send_b(near(d), i - 2, 2 + i)
            send_b(near(d), i, 4 + i, 64, 64 * (i - 2))
            cast(near(d), True)

        def advance(step):
            for yi in range(NY):
                for way in range(2):
                    if step == 3 and way != yi // 2:
                        continue
                    ring_got(step, way, yi)
                    if step < 2 or (step == 2 and way == yi // 2):
                        ring(step + 1, way, yi)

        advance(0)
        for i, d in ((4, -3), (5, 3)):
            got_b(near(d), i)
            cast(near(d), True)
        got_b(near(4), 6, 64, 0)
        got_b(near(4), 7, 64, 64)
        cast(near(4), True)
        advance(1)
        multiply(z, True)
        multiply(near(1), True)
        multiply(near(-1), True)
        advance(2)
        multiply(near(2), True)
        multiply(near(-2), True)
        multiply(near(3), True)
        multiply(near(-3), True)
        advance(3)
        multiply(near(4), True)

        order = [(y + d) % NY for d in (2, 1, 3, 0)]
        for t in (1, 0):
            rows = pl.ds(128 * t, 128)
            for yt in order:
                send(acc.at[ph, 2 * yt + 1 - k, rows], drecv.at[ph, yt, rows], (ds.at[ph, t, yt], dr.at[ph, t, yt]), partner)

        def paired(t, yt):
            rows = pl.ds(128 * t, 128)
            got(drecv.at[ph, yt, rows], (ds.at[ph, t, yt], dr.at[ph, t, yt]), partner)
            return acc[ph, 2 * yt + k, rows] + drecv[ph, yt, rows]

        for t in (1, 0):
            for d, yt in zip((2, 1, 3), order):
                ysend[ph, t, d - 1] = paired(t, yt).astype(BF16)
                part = (ysend.at[ph, t, d - 1], yrecv.at[ph, t, d - 1])
                send(*part, (ys.at[ph, t, d - 1], yr.at[ph, t, d - 1]), ypeer[d - 1])
        for t in (1, 0):
            total = paired(t, y)
            for d in (1, 3, 2):
                got(yrecv.at[ph, t, d - 1], (ys.at[ph, t, d - 1], yr.at[ph, t, d - 1]), ypeer[d - 1])
                total = total + yrecv[ph, t, d - 1].astype(F32)
            finish(t, total)

    def squared(t, total):
        block = jnp.where(tab[me_r, 34] > t, total, 0.0).astype(BF16)
        sown[t] = block
        launch(1, t, sown.at[t])
        out_ref[t] = block

    def mixed(t, total):
        value = 1.5 * xs[tab[me_r, 32 + t]].astype(F32) - 0.5 * total
        out_ref[2 + t] = jnp.where(tab[me_r, 34] > t, value, 0.0).astype(BF16)

    launch(0, 1, x_hbm.at[1])
    launch(0, 0, x_hbm.at[0])
    phase(0, squared)
    phase(1, mixed)
    for copy in pending:
        copy.wait_send()


def local(x_blocks, x_slots, x_count, s_slots, s_count):
    dma = pltpu.SemaphoreType.DMA
    vmem = pl.BlockSpec(memory_space=pltpu.VMEM)
    both = pl.pallas_call(
        kernel,
        out_shape=pltpu.VMEM((4, 128, 128), BF16),
        in_specs=[pl.BlockSpec(memory_space=pl.ANY)] * 5,
        out_specs=vmem,
        scratch_shapes=[
            pltpu.VMEM((8, 32, CAPX), I32),
            pltpu.VMEM((8, 32), I32),
            pltpu.VMEM((8, 2, 32), I32),
            pltpu.VMEM((8, 32), I32),
            pltpu.VMEM((CAPX + 1, 128, 128), BF16),
            pltpu.VMEM((2, NZ, NY, 2, 128, 128), BF16),
            pltpu.VMEM((2, 8, 256, 128), F32),
            pltpu.VMEM((2, 128, 128), BF16),
            pltpu.VMEM((2, NY, 256, 128), F32),
            pltpu.VMEM((2, 2, NY - 1, 128, 128), BF16),
            pltpu.VMEM((2, 2, NY - 1, 128, 128), BF16),
            pltpu.VMEM((8, 128), I32),
            pltpu.SMEM((8, 128), I32),
            dma, dma, dma((4,)),
            dma((2, NX)), dma((2, NY)),
            dma((2,)), dma((2,)),
            dma((2, 2, 4, NY)), dma((2, 2, 4, NY)),
            dma((2, 8)), dma((2, 8)),
            dma((2, 3, NZ)), dma((2, 3, NZ)),
            dma((2, 2, NY)), dma((2, 2, NY)),
            dma((2, 2, NY - 1)), dma((2, 2, NY - 1)),
        ],
        compiler_params=pltpu.CompilerParams(collective_id=0, has_side_effects=True),
    )(x_slots, x_count, s_slots.transpose(0, 2, 1), s_count, x_blocks.reshape(CAPX, 128, 128))
    square, result = both[:2], both[2:]
    return square[None, None], result[None, None]


def solution(mesh):
    in_specs = (P("row", "col", None, None, None), P(), P(), P(), P())
    out_specs = (P("row", "col", None, None, None), P("row", "col", None, None, None))
    return jax.shard_map(local, mesh=mesh, in_specs=in_specs, out_specs=out_specs, check_vma=False)
```

```python
import jax
import jax.numpy as jnp
from jax import lax
from jax.experimental import pallas as pl
from jax.experimental.pallas import tpu as pltpu
from jax.sharding import PartitionSpec as P

RB = 8
JW = 2
KB = 32
NY, NX, NZ = 4, 4, 8
CAPX = 42
MESH = pl.DeviceIdType.MESH
F32 = jnp.float32
BF16 = jnp.bfloat16
I32 = jnp.int32


def spread(core, z):
    half = z // 4
    z2 = z % 4
    e = (core + half) % 2
    dz = (1 - e) * (z2 // 2 * 2 - 1) + e * (((z2 + 1) // 2 - 1) * 2)
    return half, (z + dz + NZ) % NZ


def unspread(core, zl):
    w = (zl - 4 * core + NZ) % NZ
    z2 = (w // 2 + 1) % 4
    e = (w + 1) // 2 % 2
    return (core + e) % 2, z2


def find_blocks(me_r, me_c, x_slots, x_count, s_slots, s_count, tabv):
    lane = lax.broadcasted_iota(I32, (8, 128), 1)
    lane32 = lax.broadcasted_iota(I32, (8, 32), 1)

    def column(values, at):
        return jnp.sum(jnp.where(lane32 == at, values, 0), axis=1, keepdims=True)

    rows = [s_slots[:, t, :] for t in range(2)]
    xc, sc = x_count[...], s_count[...]
    so = [column(rows[t], me_c) for t in range(2)]
    bit = lane // 2 % 2
    so_lane = jnp.where(bit == 0, so[0], so[1])
    at_row = jnp.zeros((8, 128), I32)
    at_col = jnp.zeros((8, 128), I32)
    live = jnp.zeros((8, 128), I32)
    for z2 in range(4):
        c = 4 * me_r + z2
        near = x_slots[:, c, :]
        counts = (column(xc, c), column(sc, c))
        for n in range(2):
            px = near[:, n : n + 1]
            ps = column(rows[n], c)
            for ph, p, stride in ((0, px, KB), (1, ps, JW)):
                here = (lane // 4 == ph * 4 + z2) & (lane % 2 == n)
                at_row = jnp.where(here, z2 * RB + p // stride, at_row)
                at_col = jnp.where(here, p % stride, at_col)
                live = jnp.where(here, jnp.where(counts[ph] > n, 1, 0), live)
    want = jnp.where((live == 1) & (at_col == so_lane % JW), so_lane // JW * KB + at_row, -1)
    for t in range(2):
        want = jnp.where(lane == 32 + t, so[t] // JW * KB + so[t] % JW, want)
    own = x_slots[me_r, pl.ds(me_c, 1), :]
    own_count = jnp.sum(jnp.where(lane32[:1] == me_c, x_count[pl.ds(me_r, 1), :], 0), axis=1, keepdims=True)
    own = jnp.where(lax.broadcasted_iota(I32, (1, CAPX), 1) < own_count, own, -2)
    found = jnp.full((8, 128), CAPX, I32)
    for s in range(CAPX):
        found = jnp.where(want == own[:, s : s + 1], s, found)
    tabv[...] = jnp.where(lane == 34, column(sc, me_c), found)


def kernel(
    x_slots_hbm, x_count_hbm, s_slots_hbm, s_count_hbm, x_hbm, out_ref,
    x_slots, x_count, s_slots, s_count, xs, g, acc, sown, drecv, ysend, yrecv, tabv, tab,
    xsem, tsem, isem, as_, ar, bs, br, zas, zar, zbs, zbr, xbs, xbr, ds, dr, ys, yr,
):
    me_r = lax.axis_index("row")
    me_c = lax.axis_index("col")
    y, k = me_r // 2, me_r % 2
    x, z = me_c // NZ, me_c % NZ
    half, zland = spread(k, z)
    kin, z2in = unspread(k, z)

    targets = [(2 * x + half, xt * NZ + zland) for xt in range(NX)]
    landing = (2 * x + half, y * NZ + zland)
    sources = [(2 * yt + kin, y * NZ + 4 * k + z2in) for yt in range(NY)]
    zpeer = [(me_r, x * NZ + (z + d + NZ) % NZ) for d in (1, -1, 2, -2)]
    partner = (2 * y + 1 - k, me_c)
    ypeer = [(2 * ((y + d) % NY) + k, me_c) for d in range(1, NY)]

    def xpeer(dx):
        return (me_r, (x + dx + NX) % NX * NZ + z)

    barrier = pltpu.get_barrier_semaphore()
    everyone = targets + sources + zpeer + [partner] + ypeer + [xpeer(1), xpeer(-1), xpeer(2)]
    for peer in everyone:
        pl.semaphore_signal(barrier, inc=1, device_id=peer, device_id_type=MESH)
    inputs = [
        pltpu.make_async_copy(a, b, isem.at[i])
        for i, (a, b) in enumerate(
            [(x_slots_hbm, x_slots), (x_count_hbm, x_count), (s_slots_hbm, s_slots), (s_count_hbm, s_count)]
        )
    ]
    x_copy = pltpu.make_async_copy(x_hbm, xs.at[pl.ds(0, CAPX)], xsem)
    for copy in inputs + [x_copy]:
        copy.start()
    xs[CAPX] = jnp.zeros((128, 128), BF16)
    pl.semaphore_wait(barrier, len(everyone))

    nearest = [(y + d) % NY for d in (0, 1, 3, 2)]
    pending = []

    def remote(src, dst, sems, peer):
        return pltpu.make_async_remote_copy(
            src_ref=src, dst_ref=dst, send_sem=sems[0], recv_sem=sems[1],
            device_id=peer, device_id_type=MESH,
        )

    def send(src, dst, sems, peer):
        copy = remote(src, dst, sems, peer)
        copy.start()
        pending.append(copy)

    def got(dst, sems, peer):
        remote(dst, dst, sems, peer).wait_recv()

    def launch(ph, n, own):
        part = g.at[ph, zland, y, n]
        if n == 1:
            send(own, part, (bs.at[ph], br.at[ph]), landing)
            return
        for d in range(NX):
            peer = (2 * x + half, (x + d + 1) % NX * NZ + zland)
            send(own, part, (as_.at[ph, d], ar.at[ph, y]), peer)

    def phase(ph, finish):
        def block(zl, yi, n):
            return g.at[ph, zl, yi, n]

        if ph == 0:
            for copy in inputs:
                copy.wait()
            find_blocks(me_r, me_c, x_slots, x_count, s_slots, s_count, tabv)
            tab_copy = pltpu.make_async_copy(tabv, tab, tsem)
            tab_copy.start()
        for r in range(8):
            acc[ph, r] = jnp.zeros((256, 128), F32)
        if ph == 0:
            tab_copy.wait()
            x_copy.wait()

        def sign(zl):
            return 1 - 2 * (zl % 2)

        def xsems(slot, zl):
            return (xbs.at[ph, slot, zl], xbr.at[ph, slot, zl])

        def group(step, way):
            return (z + NZ - step) % NZ if way == 0 else (z + step) % NZ

        def ring(step, way, yi):
            zl = group(step, way)
            send(block(zl, yi, 0), block(zl, yi, 0), (zas.at[ph, way, step, yi], zar.at[ph, way, step, yi]), zpeer[way])

        def ring_got(step, way, yi):
            got(block(group(step + 1, way), yi, 0), (zas.at[ph, way, step, yi], zar.at[ph, way, step, yi]), zpeer[way])

        def send_b(zl, peer, at, rows=128, first=0):
            part = g.at[ph, zl, x, 1, pl.ds(first, rows)]
            send(part, part, (zbs.at[ph, at], zbr.at[ph, at]), zpeer[peer])

        def got_b(zl, at, rows=128, first=0):
            got(g.at[ph, zl, x, 1, pl.ds(first, rows)], (zbs.at[ph, at], zbr.at[ph, at]), zpeer[0])

        def cast(zl, direct=False):
            part = block(zl, x, 1)
            for slot, dx in ((2, 2), (0, sign(zl)), (1, -sign(zl))):
                if slot < 2 or direct:
                    send(part, part, xsems(slot, zl), xpeer(dx))

        def relay(zl):
            part = block(zl, (x - sign(zl) + NX) % NX, 1)
            got(part, xsems(0, zl), xpeer(1))
            send(part, part, xsems(2, zl), xpeer(sign(zl)))

        def multiply(zl, direct=False):
            if direct:
                got(block(zl, (x - sign(zl) + NX) % NX, 1), xsems(0, zl), xpeer(1))
            got(block(zl, (x + sign(zl) + NX) % NX, 1), xsems(1, zl), xpeer(1))
            got(block(zl, (x + 2) % NX, 1), xsems(2, zl), xpeer(1))
            ksrc, z2 = unspread(k, zl)

            def one(yi, carry):
                r = 2 * yi + ksrc
                base = (ph * 4 + z2) * 4
                b = [xs[tab[r, base + i]] for i in range(4)]
                left = jnp.concatenate(
                    [jnp.concatenate([b[0], b[1]], axis=1), jnp.concatenate([b[2], b[3]], axis=1)], axis=0
                )
                right = g[ph, zl, yi].reshape(256, 128)
                acc[ph, r] += jnp.dot(left, right, preferred_element_type=F32)
                return carry

            lax.fori_loop(0, NY, one, 0, unroll=True)

        def near(d):
            return (z + d + NZ) % NZ

        got(block(z, x, 1), (bs.at[ph], br.at[ph]), partner)
        for i, d in ((2, 2), (3, -2), (0, 1), (1, -1)):
            send_b(z, i, i)
        cast(z, True)
        for yi in nearest:
            got(block(z, yi, 0), (as_.at[ph, 0], ar.at[ph, yi]), partner)
            ring(0, 0, yi)
            ring(0, 1, yi)
        for i, d in ((0, -1), (1, 1)):
            got_b(near(d), i)
            cast(near(d), True)
        for i, d in ((2, -2), (3, 2)):
            got_b(near(d), i)
            send_b(near(d), i - 2, 2 + i)
            send_b(near(d), i, 4 + i, 64, 64 * (i - 2))
            cast(near(d), True)

        def advance(step):
            for place, yi in enumerate(nearest):
                for way in range(2):
                    if step == 3 and way != place // 2:
                        continue
                    ring_got(step, way, yi)
                    if step < 2 or (step == 2 and way == place // 2):
                        ring(step + 1, way, yi)

        advance(0)
        for i, d in ((4, -3), (5, 3)):
            got_b(near(d), i)
            cast(near(d), True)
        got_b(near(4), 6, 64, 0)
        got_b(near(4), 7, 64, 64)
        cast(near(4), True)
        advance(1)
        multiply(z, True)
        multiply(near(1), True)
        multiply(near(-1), True)
        advance(2)
        multiply(near(2), True)
        multiply(near(-2), True)
        multiply(near(3), True)
        multiply(near(-3), True)
        advance(3)
        multiply(near(4), True)

        order = [(y + d) % NY for d in (2, 1, 3, 0)]
        for t in (1, 0):
            rows = pl.ds(128 * t, 128)
            for yt in order:
                send(acc.at[ph, 2 * yt + 1 - k, rows], drecv.at[ph, yt, rows], (ds.at[ph, t, yt], dr.at[ph, t, yt]), partner)

        def paired(t, yt):
            rows = pl.ds(128 * t, 128)
            got(drecv.at[ph, yt, rows], (ds.at[ph, t, yt], dr.at[ph, t, yt]), partner)
            return acc[ph, 2 * yt + k, rows] + drecv[ph, yt, rows]

        for t in (1, 0):
            for d, yt in zip((2, 1, 3), order):
                ysend[ph, t, d - 1] = paired(t, yt).astype(BF16)
                part = (ysend.at[ph, t, d - 1], yrecv.at[ph, t, d - 1])
                send(*part, (ys.at[ph, t, d - 1], yr.at[ph, t, d - 1]), ypeer[d - 1])
        for t in (1, 0):
            total = paired(t, y)
            for d in (1, 3, 2):
                got(yrecv.at[ph, t, d - 1], (ys.at[ph, t, d - 1], yr.at[ph, t, d - 1]), ypeer[d - 1])
                total = total + yrecv[ph, t, d - 1].astype(F32)
            finish(t, total)

    def squared(t, total):
        block = jnp.where(tab[me_r, 34] > t, total, 0.0).astype(BF16)
        sown[t] = block
        launch(1, t, sown.at[t])
        out_ref[t] = block

    def mixed(t, total):
        value = 1.5 * xs[tab[me_r, 32 + t]].astype(F32) - 0.5 * total
        out_ref[2 + t] = jnp.where(tab[me_r, 34] > t, value, 0.0).astype(BF16)

    launch(0, 1, x_hbm.at[1])
    launch(0, 0, x_hbm.at[0])
    phase(0, squared)
    phase(1, mixed)
    for copy in pending:
        copy.wait_send()


def local(x_blocks, x_slots, x_count, s_slots, s_count):
    dma = pltpu.SemaphoreType.DMA
    vmem = pl.BlockSpec(memory_space=pltpu.VMEM)
    both = pl.pallas_call(
        kernel,
        out_shape=pltpu.VMEM((4, 128, 128), BF16),
        in_specs=[pl.BlockSpec(memory_space=pl.ANY)] * 5,
        out_specs=vmem,
        scratch_shapes=[
            pltpu.VMEM((8, 32, CAPX), I32),
            pltpu.VMEM((8, 32), I32),
            pltpu.VMEM((8, 2, 32), I32),
            pltpu.VMEM((8, 32), I32),
            pltpu.VMEM((CAPX + 1, 128, 128), BF16),
            pltpu.VMEM((2, NZ, NY, 2, 128, 128), BF16),
            pltpu.VMEM((2, 8, 256, 128), F32),
            pltpu.VMEM((2, 128, 128), BF16),
            pltpu.VMEM((2, NY, 256, 128), F32),
            pltpu.VMEM((2, 2, NY - 1, 128, 128), BF16),
            pltpu.VMEM((2, 2, NY - 1, 128, 128), BF16),
            pltpu.VMEM((8, 128), I32),
            pltpu.SMEM((8, 128), I32),
            dma, dma, dma((4,)),
            dma((2, NX)), dma((2, NY)),
            dma((2,)), dma((2,)),
            dma((2, 2, 4, NY)), dma((2, 2, 4, NY)),
            dma((2, 8)), dma((2, 8)),
            dma((2, 3, NZ)), dma((2, 3, NZ)),
            dma((2, 2, NY)), dma((2, 2, NY)),
            dma((2, 2, NY - 1)), dma((2, 2, NY - 1)),
        ],
        compiler_params=pltpu.CompilerParams(collective_id=0, has_side_effects=True),
    )(x_slots, x_count, s_slots.transpose(0, 2, 1), s_count, x_blocks.reshape(CAPX, 128, 128))
    square, result = both[:2], both[2:]
    return square[None, None], result[None, None]


def solution(mesh):
    in_specs = (P("row", "col", None, None, None), P(), P(), P(), P())
    out_specs = (P("row", "col", None, None, None), P("row", "col", None, None, None))
    return jax.shard_map(local, mesh=mesh, in_specs=in_specs, out_specs=out_specs, check_vma=False)
```
